32 devices in a mesh: batch: 8 (over z, x), head: 4 (over y, core).
Axes of the slice: x: 2, y: 2, z: 4, core: 2. Of those that a mesh axis runs over, the one named last changes fastest.
Arguments:
- features: bfloat16 [1024, 24, 512], P(('batch', 'head')), may hold values from -6 to 6
- state_h: bfloat16 [1024, 1024], P(('batch', 'head')), may hold values from -0.8984375 to 0.8984375
- state_c: bfloat16 [1024, 1024], P(('batch', 'head')), may hold values from -4 to 4
- valid: int32 [1024], P(('batch', 'head')), may hold values 0 or 1
- ends: int32 [1024, 24], P(('batch', 'head')), may hold values 0 or 1
- policy: int32 [1024, 1], P(('batch', 'head')), may hold values from 0 to 31; in each aligned block of 32 rows (0 to 31, 32 to 63, ...) at most 2 rows name the same one
- actions: int32 [1024, 16], P(('batch', 'head')), may hold values from 0 to 17
- w_input: bfloat16 [512, 4, 1024], P('batch', None, 'head'), may hold values from -0.25 to 0.25
- w_recur: bfloat16 [1024, 4, 1024], P('batch', None, 'head'), may hold values from -0.1875 to 0.1875
- lstm_bias: float32 [4, 1024], replicated, may hold values from -3 to 5
- w_hidden: bfloat16 [32, 1024, 1024], P('head'), may hold values from -0.1875 to 0.1875
- w_value: bfloat16 [32, 512], P('head'), may hold values from -0.25 to 0.25
- w_advantage: bfloat16 [32, 512, 18], P('head'), may hold values from -0.25 to 0.25
Outputs:
- q_values: float32 [1024, 16, 18], P(('batch', 'head'))
- q_taken: float32 [1024, 16], P(('batch', 'head'))
The draws below stay inside these ranges and needn't reach their ends.
Inputs may be any that keep to these rules, and one draw needn't show every extreme that they name: In the rows of one device no policy appears more than 2 times, and some policy appears exactly 2 times.
All inputs are finite; a program needn't handle non-finite values. No bound on the sum of `valid` or of `ends` on one device may be relied on, other than what follows from the above.
Results may differ from the reference program's by a relative error of at most 0.007.
Values may be sent and summed in bfloat16 or wider, within the bound.
No kernel may reach another device: no remote copies, remote signals or barrier semaphores. Data moves between devices by JAX's collectives and lax.ppermute only.
A program may use at most 128 MiB of HBM per device.

```python
import math
import jax
import jax.numpy as jnp
import numpy as np
from jax import lax

E = 512
H = 1024
HID = 512
ACTIONS = 18
POLICIES = 32
SEQ_DEV = 32
BURN = 8
LEARN = 16
CAPP = 2
STEPS = 24
SEQS = 1024


def draw_lstm_bias(key, part):
    base = jax.random.fold_in(key, 41)
    first_key, second_key = jax.random.split(base)
    others = jnp.clip(0.5 * jax.random.normal(first_key, (4, H), jnp.float32), -3.0, 3.0)
    forget = jax.random.uniform(second_key, (H,), jnp.float32, 1.5, 4.5)
    which_row = jnp.arange(4, dtype=jnp.int32)[:, None] == 1
    return jnp.where(which_row, forget[None, :], others).astype(jnp.float32)


def place_ends(values, stream_key, smallest, high):
    place = [jax.random.randint(jax.random.fold_in(stream_key, axis), (), 0, length) for axis, length in enumerate(values.shape)]
    longest = values.shape.index(max(values.shape))
    beside = place[:longest] + [(place[longest] + 1) % values.shape[longest]] + place[longest + 1:]
    return values.at[tuple(place)].set(smallest).at[tuple(beside)].set(high)


def block_scale(stream_key, dims, cuts, smallest, high):
    gain, own = 1.0, jax.random.fold_in(stream_key, 6)
    for axis_at, blocks in cuts:
        heights = jnp.exp(jax.random.uniform(jax.random.fold_in(own, axis_at), (blocks,), jnp.float32, smallest / len(cuts), high / len(cuts)))
        gain = gain * jnp.repeat(heights, dims[axis_at] // blocks).reshape([-1 if axis == axis_at else 1 for axis in range(len(dims))])
    return gain


def routed_block(rng, own, number, rows, number_of, top, bound, skew):
    ranking = jax.random.permutation(rng, number_of)
    crowded, ordinary = shares(number_of, rows * top, bound, skew, True), shares(number_of, rows * top, bound, skew, False)
    places = jnp.arange(number_of)

    def named(lengths, turn):
        used = int((lengths > 0).sum())
        fixed = max(1, used // 4)
        passed = fixed + (places - fixed + turn * (used - fixed)) % max(1, number_of - fixed)
        return jnp.zeros((number_of,), jnp.int32).at[ranking[jnp.where(places < fixed, places, passed)]].set(jnp.asarray(lengths, jnp.int32))

    lengths = jnp.where(number % 4 == 0, named(crowded, number // 4), named(ordinary, number - number // 4 - 1))
    mixed = jax.random.permutation(jax.random.fold_in(own, 3), number_of)
    donor, receiver = mixed[0:number_of // 2 * 2:2], mixed[1:number_of // 2 * 2:2]
    room = jnp.minimum(lengths[donor] - 1, bound - lengths[receiver]) // 2
    room = jnp.where((donor == ranking[0]) | (receiver == ranking[0]) | (lengths[receiver] == 0), 0, jnp.maximum(room, 0))
    passed = jax.random.randint(jax.random.fold_in(own, 4), (number_of // 2,), 0, 1 << 20) % (room + 1)
    lengths = lengths.at[donor].add(-passed).at[receiver].add(passed)
    labels = jnp.searchsorted(jnp.cumsum(lengths), jnp.arange(rows * top), side="right").astype(jnp.int32)
    table = labels.reshape(top, rows).T
    table = table[jax.random.permutation(jax.random.fold_in(own, 1), rows)]
    turn = jax.random.randint(jax.random.fold_in(own, 2), (rows, 1), 0, top)
    return jnp.take_along_axis(table, (jnp.arange(top)[None, :] + turn) % top, axis=1)


def shares(amount, total, bound, skew, full):
    weights = [(1 << 20) // math.isqrt(grade ** skew) + 1 for grade in range(1, amount + 1)]
    largest = bound if full else min(bound, max(-(-total // amount), total * weights[0] // sum(weights)))
    least = 1 if total - largest >= amount - 1 else 0
    given, surplus = [largest] + [least] * (amount - 1), total - largest - least * (amount - 1)
    while surplus > 0:
        movable = [i for i in range(1, amount) if given[i] < largest] or [i for i in range(1, amount) if given[i] < bound]
        mass, budget = sum([weights[i] for i in movable]), surplus
        for i in movable:
            extra = min(bound - given[i], max(1, budget * weights[i] // mass), surplus)
            given[i] = given[i] + extra
            surplus = surplus - extra
    return np.array(given)


def centred(own_key, dims, width, most, pieces=(), kind=jnp.bfloat16):
    gain = block_scale(own_key, dims, pieces, -0.22, 0.18) if pieces else 1.0
    result = jax.random.normal(own_key, dims, jnp.float32) * width * gain
    return jnp.minimum(jnp.maximum(result, -most), most).astype(kind)


def setup_inputs(seed: int = 0) -> dict:
    key_list = jax.random.split(jax.random.key(seed), 14)
    features = centred(key_list[0], (SEQS, STEPS, E), 1.0, 6.0, ((0, 32),))
    state_h = jnp.clip(jax.random.uniform(key_list[1], (SEQS, H), jnp.float32, -0.8984375, 0.8984375) * block_scale(key_list[1], (SEQS, H), ((0, 32),), -0.4, 0.0), -0.8984375, 0.8984375).astype(jnp.bfloat16)
    state_c = centred(key_list[2], (SEQS, H), 1.0, 4.0, ((0, 32),))
    valid = place_ends((jax.random.randint(key_list[3], (SEQS,), 0, 4) < 3).astype(jnp.int32), jax.random.fold_in(key_list[3], 1), 0, 1)
    ends = place_ends((jax.random.randint(key_list[4], (SEQS, STEPS), 0, 12) < 1).astype(jnp.int32), jax.random.fold_in(key_list[4], 1), 0, 1)
    policy_keys = jax.random.split(jax.random.fold_in(key_list[5], 1), SEQS // SEQ_DEV)
    policy_turns = jax.random.permutation(jax.random.fold_in(key_list[5], 3), SEQS // SEQ_DEV)
    policy = jax.vmap(lambda own, number: routed_block(jax.random.fold_in(key_list[5], 2), own, number, SEQ_DEV, POLICIES, 1, CAPP, 2))(policy_keys, policy_turns).reshape((SEQS, 1))
    actions = place_ends(jax.random.randint(key_list[6], (SEQS, LEARN), 0, ACTIONS), jax.random.fold_in(key_list[6], 1), 0, ACTIONS - 1).astype(jnp.int32)
    w_input = centred(key_list[7], (E, 4, H), E ** -0.5, 0.25, ((0, 8), (2, 4)))
    w_recur = centred(key_list[8], (H, 4, H), H ** -0.5, 0.1875, ((0, 8), (2, 4)))
    lstm_bias = draw_lstm_bias(jax.random.fold_in(key_list[13], 71), 0)
    w_hidden = centred(key_list[10], (POLICIES, H, 2 * HID), H ** -0.5, 0.1875, ((0, 4),))
    w_value = centred(key_list[11], (POLICIES, HID), HID ** -0.5, 0.25, ((0, 4),))
    w_advantage = centred(key_list[12], (POLICIES, HID, ACTIONS), HID ** -0.5, 0.25, ((0, 4),))
    return {"features": features, "state_h": state_h, "state_c": state_c, "valid": valid, "ends": ends, "policy": policy, "actions": actions, "w_input": w_input, "w_recur": w_recur, "lstm_bias": lstm_bias, "w_hidden": w_hidden, "w_value": w_value, "w_advantage": w_advantage}


def reference(features, state_h, state_c, valid, ends, policy, actions, w_input, w_recur, lstm_bias, w_hidden, w_value, w_advantage):
    keep_start = valid.astype(jnp.float32)[:, None]
    hidden_state = (state_h.astype(jnp.float32) * keep_start).astype(jnp.bfloat16)
    cell_state = state_c.astype(jnp.float32) * keep_start
    time_major = features.transpose(1, 0, 2)
    keeps = 1.0 - ends.astype(jnp.float32).T
    w_in_flat = w_input.reshape(E, 4 * H)
    w_rec_flat = w_recur.reshape(H, 4 * H)

    def advance(carry, inputs):
        hidden_state, cell_state = carry
        feat_t, keep_t = inputs
        hidden_state = (hidden_state.astype(jnp.float32) * keep_t[:, None]).astype(jnp.bfloat16)
        cell_state = cell_state * keep_t[:, None]
        gates = jnp.dot(feat_t, w_in_flat, preferred_element_type=jnp.float32)
        gates = gates + jnp.dot(hidden_state, w_rec_flat, preferred_element_type=jnp.float32)
        gates = gates.reshape(-1, 4, H) + lstm_bias
        cell_state = jax.nn.sigmoid(gates[:, 1]) * cell_state + jax.nn.sigmoid(gates[:, 0]) * jnp.tanh(gates[:, 2])
        hidden_state = (jax.nn.sigmoid(gates[:, 3]) * jnp.tanh(cell_state)).astype(jnp.bfloat16)
        return (hidden_state, cell_state), hidden_state

    _, outputs = lax.scan(advance, (hidden_state, cell_state), (time_major, keeps))
    learned = outputs[BURN:].transpose(1, 0, 2)

    def one_head(item):
        rows, which = item
        mid = jnp.maximum(jnp.dot(rows, w_hidden[which], preferred_element_type=jnp.float32), 0.0).astype(jnp.bfloat16)
        value = jnp.dot(mid[:, :HID], w_value[which], preferred_element_type=jnp.float32)
        advantage = jnp.dot(mid[:, HID:], w_advantage[which], preferred_element_type=jnp.float32)
        return value[:, None] + advantage - jnp.mean(advantage, axis=-1, keepdims=True)

    q_values = lax.map(one_head, (learned, policy[:, 0].astype(jnp.int32)))
    chosen = actions[:, :, None] == jnp.arange(ACTIONS, dtype=jnp.int32)[None, None, :]
    q_taken = jnp.sum(jnp.where(chosen, q_values, 0.0), axis=-1)
    return q_values, q_taken
```

```python
import jax
import jax.numpy as jnp
from jax import lax
from jax.experimental import pallas as pl
from jax.experimental.pallas import tpu as pltpu
from jax.sharding import PartitionSpec as P

AXES = ("batch", "head")
CAPP = 2
LANES = 128
SPAN = 32


class Moves:
    def __init__(self, batches, heads):
        self.inner = 2 if batches % 2 == 0 else 1
        self.cores = 2 if heads % 2 == 0 else 1
        self.ring_len = batches // self.inner
        self.heads = heads
        self.total = batches * heads
        self.batches = batches

    def xor_batch(self, a, m):
        h = self.heads
        return lax.ppermute(a, AXES, [(i, ((i // h) ^ m) * h + i % h) for i in range(self.total)])

    def xor_head(self, a, m):
        h = self.heads
        return lax.ppermute(a, AXES, [(i, (i // h) * h + ((i % h) ^ m)) for i in range(self.total)])

    def ring(self, a):
        step = self.inner * self.heads
        return lax.ppermute(a, AXES, [(i, (i + step) % self.total) for i in range(self.total)])

    def x(self, a):
        return self.xor_batch(a, 1)

    def y(self, a):
        return self.xor_head(a, 2)

    def c(self, a):
        return self.xor_head(a, 1)


def sigmoid(v):
    return 0.5 * jnp.tanh(0.5 * v) + 0.5


def gather_items(move, item):
    found = []
    gates = item.shape[0]
    half = gates // 2
    own = item
    for r in range(move.ring_len):
        nxt = move.ring(own) if r + 1 < move.ring_len else None
        xo = move.x(own)
        yo = move.y(own)
        yx = move.y(xo[:half])
        xy = move.x(yo[half:])
        for arr, xb, hb, g0 in ((own, 0, 0, 0), (xo, 1, 0, 0), (yo, 0, 2, 0), (yx, 1, 2, 0), (xy, 1, 2, half)):
            found.append((arr, r, xb, hb, g0))
            found.append((move.c(arr), r, xb, hb ^ 1, g0))
        own = nxt
    return found


def lstm_kernel(info, dims, *refs):
    steps, learn, rows, width_e, width_h, heads, quarter, rows_in, rows_rec, ring_len, inner = dims
    n = len(info)
    where, pieces = refs[0], refs[1 : n + 1]
    feats, start_h, start_c, keeps, bias, out, w_in, w_rec, pre, state_h, state_c, sem_in, sem_rec = refs[n + 1 :]
    burn = steps - learn
    zo, xb, hd = where[0], where[1], where[2]

    copies_in, copies_rec = [], []
    for piece, (r, xbit, hbits, g0) in zip(pieces, info):
        gates = piece.shape[0]
        source = lax.rem(zo + ring_len - r, ring_len)
        block = source * inner + jnp.bitwise_xor(xb, xbit)
        col = jnp.bitwise_xor(hd, hbits)
        copies_in.append(
            pltpu.make_async_copy(
                piece.at[:, pl.ds(0, rows_in), :],
                w_in.at[col, pl.ds(g0, gates), pl.ds(pl.multiple_of(block * rows_in, rows_in), rows_in), :],
                sem_in,
            )
        )
        copies_rec.append(
            pltpu.make_async_copy(
                piece.at[:, pl.ds(rows_in, rows_rec), :],
                w_rec.at[col, pl.ds(g0, gates), pl.ds(pl.multiple_of(block * rows_rec, rows_rec), rows_rec), :],
                sem_rec,
            )
        )
    for copy in copies_in:
        copy.start()
    for copy in copies_rec:
        copy.start()
    state_h[...] = start_h[...]
    state_c[...] = start_c[...]
    for copy in copies_in:
        copy.wait()

    def project(index, carry):
        col, gate = index // 4, lax.rem(index, 4)
        pre[col, gate] = (
            jnp.dot(feats[...], w_in[col, gate], preferred_element_type=jnp.float32) + bias[col, gate]
        )
        return carry

    lax.fori_loop(0, heads * 4, project, 0)
    for copy in copies_rec:
        copy.wait()

    def advance(t, carry):
        keep = keeps[t]
        keep_wide = jnp.concatenate([keep] * (quarter // LANES), axis=1)
        keep_all = jnp.concatenate([keep] * (width_h // LANES), axis=1)
        h = (state_h[...].astype(jnp.float32) * keep_all).astype(jnp.bfloat16)
        span = pl.ds(pl.multiple_of(t * rows, rows), rows)
        for col in range(heads):
            lanes = pl.ds(col * quarter, quarter)
            gate = [
                pre[col, k, span, :] + jnp.dot(h, w_rec[col, k], preferred_element_type=jnp.float32)
                for k in range(4)
            ]
            c = state_c[:, lanes] * keep_wide
            c = sigmoid(gate[1]) * c + sigmoid(gate[0]) * jnp.tanh(gate[2])
            state_c[:, lanes] = c
            state_h[:, lanes] = (sigmoid(gate[3]) * jnp.tanh(c)).astype(jnp.bfloat16)

        @pl.when(t >= burn)
        def _():
            out[t - burn] = state_h[...]

        return carry

    lax.fori_loop(0, steps, advance, 0)


def run_lstm(found, where, feats, start_h, start_c, keeps, bias, dims):
    steps, learn, rows, width_e, width_h, heads, quarter, rows_in, rows_rec, ring_len, inner = dims
    info = tuple(f[1:] for f in found)
    anywhere = pl.BlockSpec(memory_space=pl.ANY)
    vmem = pl.BlockSpec(memory_space=pltpu.VMEM)
    return pl.pallas_call(
        lambda *refs: lstm_kernel(info, dims, *refs),
        out_shape=jax.ShapeDtypeStruct((learn, rows, width_h), jnp.bfloat16),
        in_specs=[pl.BlockSpec(memory_space=pltpu.SMEM)] + [anywhere] * len(found) + [vmem] * 5,
        out_specs=vmem,
        scratch_shapes=[
            pltpu.VMEM((heads, 4, width_e, quarter), jnp.bfloat16),
            pltpu.VMEM((heads, 4, width_h, quarter), jnp.bfloat16),
            pltpu.VMEM((heads, 4, steps * rows, quarter), jnp.float32),
            pltpu.VMEM((rows, width_h), jnp.bfloat16),
            pltpu.VMEM((rows, width_h), jnp.float32),
            pltpu.SemaphoreType.DMA,
            pltpu.SemaphoreType.DMA,
        ],
        compiler_params=pltpu.CompilerParams(vmem_limit_bytes=56 * 1024 * 1024),
        name="recurrence",
    )(where, *[f[0] for f in found], feats, start_h, start_c, keeps, bias)


def heads_kernel(dims, *refs):
    group, local, parts, eight = dims
    hs, (pick, w_hidden, w_out, mixer, out, rows, total) = refs[:group], refs[group:]
    p = pl.program_id(0)

    @pl.when(p == 0)
    def _():
        for k in range(group):
            for q in range(parts):
                block = hs[k][pl.ds(q * eight, eight)]
                block = block.reshape(block.shape[0] * block.shape[1], block.shape[2])
                got = jnp.dot(pick[k], block, preferred_element_type=jnp.float32).astype(jnp.bfloat16)
                rows[:, q, k] = got.reshape(local, eight * CAPP, block.shape[1])

    mine = rows[p]
    mine = mine.reshape(parts * group * eight * CAPP, mine.shape[-1])
    mid = jnp.maximum(jnp.dot(mine, w_hidden[0], preferred_element_type=jnp.float32), 0.0).astype(jnp.bfloat16)
    part = jnp.dot(mid, w_out[0], preferred_element_type=jnp.float32)
    g = p // (LANES // SPAN)

    @pl.when(lax.rem(p, LANES // SPAN) == 0)
    def _():
        total[...] = part

    @pl.when(lax.rem(p, LANES // SPAN) != 0)
    def _():
        total[...] += part

    @pl.when(lax.rem(p, LANES // SPAN) == LANES // SPAN - 1)
    def _():
        q_all = jnp.dot(total[...], mixer[...], precision=lax.Precision.HIGHEST, preferred_element_type=jnp.float32)
        q_all = q_all.astype(jnp.bfloat16).reshape(parts, group, eight * CAPP, LANES)
        for k in range(group):
            out[k, g] = q_all[:, k].reshape(parts * eight * CAPP, LANES)


def run_heads(hs, pick, w_hidden, w_out, mixer):
    group = len(hs)
    local, width_h, width_m = w_hidden.shape
    learn, rows, _ = hs[0].shape
    eight = pick.shape[2] // rows
    parts = learn // eight
    vmem = pl.BlockSpec(memory_space=pltpu.VMEM)
    per = LANES // SPAN
    dims = (group, local, parts, eight)
    return pl.pallas_call(
        lambda *refs: heads_kernel(dims, *refs),
        grid=(local,),
        out_shape=jax.ShapeDtypeStruct((group, local // per, learn * CAPP, LANES), jnp.bfloat16),
        in_specs=[vmem] * (group + 1)
        + [
            pl.BlockSpec((1, width_h, width_m), lambda p: (p, 0, 0)),
            pl.BlockSpec((1, width_m, LANES), lambda p: (p, 0, 0)),
            vmem,
        ],
        out_specs=vmem,
        scratch_shapes=[
            pltpu.VMEM((local, parts, group, eight * CAPP, width_h), jnp.bfloat16),
            pltpu.VMEM((parts * group * eight * CAPP, LANES), jnp.float32),
        ],
        compiler_params=pltpu.CompilerParams(
            vmem_limit_bytes=40 * 1024 * 1024, dimension_semantics=("arbitrary",)
        ),
        name="policy_heads",
    )(*hs, pick, w_hidden, w_out, mixer)


def final_kernel(dims, place, q0, q1, q2, q3, out, wide):
    rows, learn, actions = dims
    for k, q in enumerate((q0, q1, q2, q3)):
        wide[k] = q[...].astype(jnp.float32)
    for i in range(rows):
        k, g, turn, j = place[0, i], place[1, i], place[2, i], place[3, i]
        got = wide[k, g, pl.ds(j, learn, stride=CAPP), :]
        out[i] = pltpu.roll(got, turn, axis=1)[:, :actions]


def run_final(place, qs, rows, learn, actions):
    vmem = pl.BlockSpec(memory_space=pltpu.VMEM)
    return pl.pallas_call(
        lambda *refs: final_kernel((rows, learn, actions), *refs),
        out_shape=jax.ShapeDtypeStruct((rows, learn, actions), jnp.float32),
        in_specs=[pl.BlockSpec(memory_space=pltpu.SMEM)] + [vmem] * 4,
        out_specs=vmem,
        scratch_shapes=[pltpu.VMEM((4,) + qs[0].shape, jnp.float32)],
        name="final_pick",
    )(place, *qs)


def shards(
    features, state_h, state_c, valid, ends, policy, actions, w_input, w_recur, lstm_bias, w_hidden, w_value, w_advantage
):
    batches, heads = lax.axis_size("batch"), lax.axis_size("head")
    rows, steps, width_e = features.shape
    width_h = state_h.shape[1]
    learn = actions.shape[1]
    n_act = w_advantage.shape[2]
    rows_in, _, quarter = w_input.shape
    rows_rec = w_recur.shape[0]
    local = w_hidden.shape[0]
    branch = w_value.shape[1]
    move = Moves(batches, heads)
    b, hd = lax.axis_index("batch"), lax.axis_index("head")

    item = jnp.concatenate([w_input.transpose(1, 0, 2), w_recur.transpose(1, 0, 2)], axis=1)
    found = gather_items(move, item)

    pol = policy[:, 0].astype(jnp.int32)
    pol_y = move.y(policy)
    pol_c = move.c(policy)
    pol_d = move.c(pol_y)
    pols = jnp.stack([pol, pol_c[:, 0], pol_y[:, 0], pol_d[:, 0]])

    def ranks(v):
        place = jnp.arange(rows, dtype=jnp.int32)
        same = (v[..., :, None] == v[..., None, :]) & (place[None, :] < place[:, None])
        return jnp.sum(same.astype(jnp.int32), axis=-1)

    rank = ranks(pols)
    slot = jnp.arange(local, dtype=jnp.int32)[None, :, None, None]
    turn_of = jnp.arange(CAPP, dtype=jnp.int32)[None, None, :, None]
    select = ((pols[:, None, None, :] == hd * local + slot) & (rank[:, None, None, :] == turn_of)).astype(jnp.bfloat16)
    eight = learn // 2
    eye = jnp.eye(eight, dtype=jnp.bfloat16)
    pick = (select[:, :, None, :, None, :] * eye[None, None, :, None, :, None]).reshape(
        4, local * eight * CAPP, eight * rows
    )

    per = LANES // SPAN
    out_cols = jnp.concatenate(
        [
            jnp.concatenate([jnp.zeros((local, branch, n_act), jnp.bfloat16), w_value[:, :, None]], axis=2),
            jnp.concatenate([w_advantage, jnp.zeros((local, branch, 1), jnp.bfloat16)], axis=2),
        ],
        axis=1,
    )
    out_cols = jnp.pad(out_cols, ((0, 0), (0, 0), (0, SPAN - n_act - 1)))
    lane_of = jnp.arange(per, dtype=jnp.int32)[None, :, None, None]
    which = (jnp.arange(local, dtype=jnp.int32) % per)[:, None, None, None]
    w_out = jnp.where(lane_of == which, out_cols[:, None], 0)
    w_out = w_out.transpose(0, 2, 1, 3).reshape(local, 2 * branch, LANES)
    lane = jnp.arange(LANES, dtype=jnp.int32)
    col, grp = lane % SPAN, lane // SPAN
    same_group = grp[:, None] == grp[None, :]
    is_act, is_val = (col < n_act)[:, None], (col == n_act)[:, None]
    mixer = (
        (lane[:, None] == lane[None, :]).astype(jnp.float32)
        - jnp.where(is_act & same_group, 1.0 / n_act, 0.0)
        + jnp.where(is_val & same_group, 1.0, 0.0)
    )
    mixer = jnp.where((col < n_act)[None, :], mixer, 0.0)

    keep_start = valid.astype(jnp.bfloat16)[:, None]
    start_h = state_h * keep_start
    start_c = (state_c * keep_start).astype(jnp.float32)
    feats = features.transpose(1, 0, 2).reshape(steps * rows, width_e)
    keeps = jnp.broadcast_to((1.0 - ends.astype(jnp.float32)).T[:, :, None], (steps, rows, LANES))
    bias = lstm_bias.reshape(4, heads, 1, quarter).transpose(1, 0, 2, 3)
    where = jnp.stack([b // move.inner, b % move.inner, hd]).astype(jnp.int32)
    dims = (steps, learn, rows, width_e, width_h, heads, quarter, rows_in, rows_rec, move.ring_len, move.inner)
    hs = run_lstm(found, where, feats, start_h, start_c, keeps, bias, dims)

    hs_y = move.y(hs)
    hs_c = move.c(hs)
    hs_d = move.c(hs_y)
    q = run_heads((hs, hs_c, hs_y, hs_d), pick, w_hidden, w_out, mixer)

    q_back = move.y(q[2:])
    q1 = move.c(q[1])
    q3 = move.c(q_back[1])
    owner, lp = pol // local, pol % local
    place = jnp.stack(
        [jnp.bitwise_xor(owner, hd), lp // per, (LANES - SPAN * (lp % per)) % LANES, rank[0]]
    ).astype(jnp.int32)
    q_values = run_final(place, (q[0], q1, q_back[0], q3), rows, learn, n_act)
    chosen = actions[:, :, None] == jnp.arange(n_act, dtype=jnp.int32)[None, None, :]
    q_taken = jnp.sum(jnp.where(chosen, q_values, 0.0), axis=-1)
    return (q_values, q_taken)


def solution(mesh):
    return jax.shard_map(
        shards,
        mesh=mesh,
        in_specs=(
            P(("batch", "head"), None, None),
            P(("batch", "head"), None),
            P(("batch", "head"), None),
            P(("batch", "head")),
            P(("batch", "head"), None),
            P(("batch", "head"), None),
            P(("batch", "head"), None),
            P("batch", None, "head"),
            P("batch", None, "head"),
            P(),
            P("head", None, None),
            P("head", None),
            P("head", None, None),
        ),
        out_specs=(P(("batch", "head"), None, None), P(("batch", "head"), None)),
        check_vma=False,
    )
```
